32 devices in a mesh: ctx: 8 (over y, x, core), head: 4 (over z).
Axes of the slice: x: 2, y: 2, z: 4, core: 2. Of those that a mesh axis runs over, the one named last changes fastest.
Arguments:
- tokens: bfloat16 [1024, 4096], P('ctx'), may hold values from -8 to 8
- w_query: bfloat16 [4096, 4096], P(None, 'head'), may hold values from -1 to 1
- w_key: bfloat16 [4096, 1024], P(None, 'head'), may hold values from -1 to 1
- w_value: bfloat16 [4096, 1024], P(None, 'head'), may hold values from -0.09375 to 0.09375
- w_out: bfloat16 [4096, 4096], P('head'), may hold values from -0.09375 to 0.09375
- doc_ids: int32 [1024], P('ctx'), may hold values from 0 to 7, never falling along the last dimension, each value on 1 to 640 neighbouring positions
Outputs:
- mixed: bfloat16 [1024, 4096], P('ctx', 'head')
The draws below stay inside these ranges and needn't reach their ends.
Inputs may be any that keep to these rules, and one draw needn't show every extreme that they name: doc_ids never fall along the context; each document has 1 to 640 tokens and one has exactly 640.
All inputs are finite; a program needn't handle non-finite values.
Results may differ from the reference program's by a relative error of at most 0.011.
Values may be sent and summed in bfloat16 or wider, within the bound.
A program may use at most 128 MiB of HBM per device.

```python
import math
import jax
import jax.numpy as jnp
import numpy as np
from jax import lax

D = 4096
QH = 32
KVH = 8
HD = 128
TOKENS = 1024
DOC_MOST = 640
DOCS = 8
N_HEAD = 4


def drawn_weight(key, head_count, salt_value):
    entries = jax.random.truncated_normal(jax.random.fold_in(key, salt_value), -6.0, 6.0, (D, head_count * HD), jnp.float32) * D ** (-0.5)
    return entries.astype(jnp.bfloat16)


def draw_w_query(key, part):
    return drawn_weight(key, QH, 11)


def draw_w_key(key, part):
    return drawn_weight(key, KVH, 12)


def draw_tokens(key, part):
    values_drawn = jax.random.truncated_normal(jax.random.fold_in(key, 13), -6.0, 6.0, (TOKENS, D), jnp.float32)
    return values_drawn.astype(jnp.bfloat16)


def level_of(key, extent, shards, smallest, top_value):
    factor_of = 1.0
    for position, parts in shards:
        draws = jax.random.uniform(jax.random.fold_in(jax.random.fold_in(key, 6), position), (parts,), jnp.float32, smallest / len(shards), top_value / len(shards))
        factor_of = factor_of * jnp.repeat(jnp.exp(draws), extent[position] // parts).reshape((-1,) + (1,) * (len(extent) - 1 - position))
    return factor_of


def profile(amount, total, most, skew):
    loads = [(1 << 20) // math.isqrt(rank ** skew) + 1 for rank in range(2, amount + 1)]
    surplus, given = total - most - (amount - 1), [1] * (amount - 1)
    while surplus > 0:
        free = [i for i in range(amount - 1) if given[i] < most]
        whole, left = sum([loads[i] for i in free]), surplus
        for i in free:
            addition = min(most - given[i], max(1, left * loads[i] // whole), surplus)
            given[i] = given[i] + addition
            surplus = surplus - addition
    return np.array([most] + given)


def uneven_parts(key, count, total, bound, skew):
    if count == 2:
        one = jax.random.randint(key, (), max(1, total - bound), min(bound, total - 1) + 1)
        return jnp.stack([one, total - one])
    lengths = jnp.asarray(profile(count, total, bound, skew), jnp.int32)
    twos = (count - 1) // 2
    giver, taker = lengths[1:1 + 2 * twos:2], lengths[2:2 + 2 * twos:2]
    room = jnp.minimum(giver - 1, bound - taker)
    shifted = jax.random.randint(jax.random.fold_in(key, 1), (twos,), 0, 1 << 20) % (room + 1)
    lengths = lengths.at[1:1 + 2 * twos:2].set(giver - shifted).at[2:2 + 2 * twos:2].set(taker + shifted)
    return lengths[jax.random.permutation(jax.random.fold_in(key, 2), count)]


def scatter_about(own_key, extent, deviation, limit, pieces=(), kind=jnp.bfloat16):
    values = jax.random.normal(own_key, extent, jnp.float32) * deviation
    if len(pieces) > 0:
        values = level_of(own_key, extent, pieces, -0.22, 0.18) * values
    return jnp.clip(values, min=-limit, max=limit).astype(kind)


def setup_inputs(seed: int = 0) -> dict:
    key_of = jax.random.split(jax.random.key(seed), 7)
    return {
        "tokens": draw_tokens(jax.random.fold_in(key_of[6], 71), 0),
        "w_query": draw_w_query(jax.random.fold_in(key_of[6], 71), 0),
        "w_key": draw_w_key(jax.random.fold_in(key_of[6], 71), 0),
        "w_value": scatter_about(key_of[3], (D, KVH * HD), D ** -0.5, 0.09375, ((1, 4),)),
        "w_out": scatter_about(key_of[4], (QH * HD, D), (QH * HD) ** -0.5, 0.09375, ((0, 4),)),
        "doc_ids": jnp.searchsorted(jnp.cumsum(uneven_parts(key_of[5], DOCS, TOKENS, DOC_MOST, 2)), jnp.arange(TOKENS), side="right").astype(jnp.int32),
    }


def rotate(vectors, places):
    half_dim = vectors.shape[-1] // 2
    freqs = 500000.0 ** (-2.0 * jnp.arange(half_dim, dtype=jnp.float32) / vectors.shape[-1])
    angles = places.astype(jnp.float32)[:, None] * freqs[None, :]
    cosine = jnp.cos(angles)[:, None, :]
    sine = jnp.sin(angles)[:, None, :]
    first_half = vectors[..., :half_dim]
    second_half = vectors[..., half_dim:]
    return jnp.concatenate([first_half * cosine - second_half * sine, second_half * cosine + first_half * sine], axis=-1)

def reference(tokens, w_query, w_key, w_value, w_out, doc_ids):
    count = tokens.shape[0]
    places = jnp.arange(count, dtype=jnp.int32)
    queries = rotate(jnp.dot(tokens, w_query, preferred_element_type=jnp.float32).reshape(count, QH, HD), places).astype(jnp.bfloat16)
    keys_all = rotate(jnp.dot(tokens, w_key, preferred_element_type=jnp.float32).reshape(count, KVH, HD), places).astype(jnp.bfloat16)
    values_all = jnp.dot(tokens, w_value, preferred_element_type=jnp.float32).astype(jnp.bfloat16).reshape(count, KVH, HD)
    group_size = QH // KVH
    queries = queries.reshape(count, KVH, group_size, HD)
    block_rows = math.gcd(512, count)
    window = DOC_MOST + block_rows
    keys_pad = jnp.concatenate([jnp.zeros((DOC_MOST, KVH, HD), jnp.bfloat16), keys_all], axis=0)
    values_pad = jnp.concatenate([jnp.zeros((DOC_MOST, KVH, HD), jnp.bfloat16), values_all], axis=0)
    docs_pad = jnp.concatenate([jnp.full((DOC_MOST,), -1, jnp.int32), doc_ids], axis=0)
    score_scale = 1.0 / math.sqrt(HD)

    def one_block(block):
        q_start = (block * block_rows).astype(jnp.int32)
        q_block = lax.dynamic_slice_in_dim(queries, q_start, block_rows, 0).astype(jnp.float32)
        q_docs = lax.dynamic_slice_in_dim(doc_ids, q_start, block_rows, 0)
        q_index = q_start + jnp.arange(block_rows, dtype=jnp.int32)
        k_block = lax.dynamic_slice_in_dim(keys_pad, q_start, window, 0).astype(jnp.float32)
        v_block = lax.dynamic_slice_in_dim(values_pad, q_start, window, 0).astype(jnp.float32)
        k_docs = lax.dynamic_slice_in_dim(docs_pad, q_start, window, 0)
        k_index = q_start - DOC_MOST + jnp.arange(window, dtype=jnp.int32)
        allowed = (k_docs[None, :] == q_docs[:, None]) & (k_index[None, :] <= q_index[:, None])
        scores = jnp.einsum('tjgd,njd->jgtn', q_block, k_block) * score_scale
        scores = jnp.where(allowed, scores, -1e+30)
        top = lax.optimization_barrier(jnp.max(scores, axis=-1, keepdims=True))
        weights = jnp.exp(scores - top) * allowed.astype(jnp.float32)
        total = lax.optimization_barrier(jnp.sum(weights, axis=-1))
        summed = jnp.einsum('jgtn,njd->jgtd', weights.astype(jnp.bfloat16).astype(jnp.float32), v_block)
        result = summed / total[..., None]
        return jnp.transpose(result, (2, 0, 1, 3)).reshape(block_rows, QH * HD).astype(jnp.bfloat16)
    attended = lax.map(one_block, jnp.arange(count // block_rows, dtype=jnp.int32)).reshape(count, QH * HD)
    group_cols = QH * HD // N_HEAD
    mixed = jnp.zeros((count, D), jnp.float32)
    for group in range(N_HEAD):
        partial_value = jnp.dot(attended[:, group * group_cols:(group + 1) * group_cols], w_out[group * group_cols:(group + 1) * group_cols], preferred_element_type=jnp.float32).astype(jnp.bfloat16)
        partial_value = lax.optimization_barrier(partial_value)
        mixed = mixed + partial_value.astype(jnp.float32)
    return mixed.astype(jnp.bfloat16)
```

```python
import functools
import math

import jax
import jax.numpy as jnp
import numpy as np
from jax import lax
from jax.experimental import pallas as pl
from jax.experimental.pallas import tpu as pltpu
from jax.sharding import PartitionSpec as P

HD = 128
STEPS = 4
SUB = 2
MESH = pl.DeviceIdType.MESH


def kernel(
    n_ctx, n_head,
    tokens, w_query, w_key, w_value, w_out, docs, freqs, out,
    tok, wq, wk, wv, wo, freq, doc_all, kv, q_acc, kv_acc, q, cos_ref, sin_ref, doc_q,
    sc, top, tot, acc, att, part, rbuf,
    tok_sem, wq_sem, wk_sem, wv_sem, wo_sem, small_sem,
    kv_send, kv_fwd, kv_recv, part_send, part_recv,
):
    rows = tokens.shape[0]
    kv_heads = w_key.shape[1] // HD
    heads = w_query.shape[1] // HD
    group = heads // kv_heads
    kv_width = kv_heads * HD
    chips = n_ctx // 2
    me = lax.axis_index("ctx")
    z = lax.axis_index("head")
    core = lax.rem(me, 2)
    chip = me // 2
    partner = me + 1 - 2 * core
    step_rows = wq.shape[1]
    piece = wo.shape[2]

    def tok_copy(c):
        return pltpu.make_async_copy(
            tokens.at[:, pl.ds(pl.multiple_of(c * step_rows, step_rows), step_rows)],
            tok.at[c], tok_sem.at[c])

    def rows_copy(src, dst, sem, c):
        return pltpu.make_async_copy(
            src.at[pl.ds(pl.multiple_of(c * step_rows, step_rows), step_rows), :],
            dst.at[c], sem.at[c])

    def wo_copy(p):
        return pltpu.make_async_copy(
            w_out.at[:, pl.ds(pl.multiple_of(p * piece, piece), piece)], wo.at[p], wo_sem.at[p])

    doc_copy = pltpu.make_async_copy(docs, doc_all.at[me], small_sem.at[0])
    freq_copy = pltpu.make_async_copy(freqs, freq, small_sem.at[1])

    def piece_of(k):
        return jnp.where(z < n_head // 2, n_head * SUB - 1 - k, k)

    doc_copy.start()
    freq_copy.start()
    for c in range(STEPS):
        tok_copy(c).start()
        rows_copy(w_key, wk, wk_sem, c).start()
        rows_copy(w_value, wv, wv_sem, c).start()
    rows_copy(w_query, wq, wq_sem, 0).start()

    barrier = pltpu.get_barrier_semaphore()

    def greet(c, carry):
        @pl.when(c != chip)
        def _():
            pl.semaphore_signal(
                barrier, inc=1, device_id={"ctx": c * 2 + core}, device_id_type=MESH)
        return carry

    lax.fori_loop(0, chips, greet, 0)
    pl.semaphore_signal(barrier, inc=1, device_id={"ctx": partner}, device_id_type=MESH)

    @pl.when(z > 0)
    def _():
        pl.semaphore_signal(barrier, inc=1, device_id={"head": z - 1}, device_id_type=MESH)

    @pl.when(z < n_head - 1)
    def _():
        pl.semaphore_signal(barrier, inc=1, device_id={"head": z + 1}, device_id_type=MESH)

    freq_copy.wait()
    doc_copy.wait()
    places = (me * rows + lax.broadcasted_iota(jnp.int32, (rows, HD), 0)).astype(jnp.float32)
    angles = places * freq[...]
    lane = lax.broadcasted_iota(jnp.int32, (rows, HD), 1)
    cos_ref[...] = jnp.cos(angles)
    sine = jnp.sin(angles)
    sin_ref[...] = jnp.where(lane < HD // 2, -sine, sine)
    doc_q[...] = jnp.broadcast_to(doc_all[me].astype(jnp.float32), (rows, rows)).T

    def rotated(x):
        return (x * cos_ref[...] + pltpu.roll(x, HD // 2, 1) * sin_ref[...]).astype(jnp.bfloat16)

    kv_acc[...] = jnp.zeros_like(kv_acc)

    def kv_step(c, carry):
        tok_copy(c).wait()
        rows_copy(w_key, wk, wk_sem, c).wait()
        rows_copy(w_value, wv, wv_sem, c).wait()

        @pl.when(c > 0)
        def _():
            rows_copy(w_query, wq, wq_sem, c).start()
        kv_acc[:, :kv_width] += jnp.dot(tok[c], wk[c], preferred_element_type=jnp.float32)
        kv_acc[:, kv_width:] += jnp.dot(tok[c], wv[c], preferred_element_type=jnp.float32)
        return carry

    lax.fori_loop(0, STEPS, kv_step, 0)
    for h in range(kv_heads):
        kv[me, :, h * HD:(h + 1) * HD] = rotated(kv_acc[:, h * HD:(h + 1) * HD])
    kv[me, :, kv_width:] = kv_acc[:, kv_width:].astype(jnp.bfloat16)

    pl.semaphore_wait(
        barrier,
        chips + (z > 0).astype(jnp.int32) + (z < n_head - 1).astype(jnp.int32))

    def block_copies(block, sems, slot, target):
        return [
            pltpu.make_async_remote_copy(
                src_ref=ref.at[block], dst_ref=ref.at[block],
                send_sem=sems.at[i, slot], recv_sem=kv_recv.at[i, block],
                device_id={"ctx": target}, device_id_type=MESH)
            for i, ref in enumerate((kv, doc_all))
        ]

    def send_one(i, carry):
        c = chips - 1 - i
        for copy in block_copies(me, kv_send, c, c * 2 + core):
            copy.start()
        return carry

    lax.fori_loop(0, chips - 1 - chip, send_one, 0)

    @pl.when(core == 0)
    def _():
        for copy in block_copies(me, kv_send, chip, partner):
            copy.start()

    q_acc[...] = jnp.zeros_like(q_acc)

    def q_step(c, carry):
        rows_copy(w_query, wq, wq_sem, c).wait()
        for i in range(n_head * SUB // STEPS):
            wo_copy(piece_of(c * (n_head * SUB // STEPS) + i)).start()
        q_acc[...] += jnp.dot(tok[c], wq[c], preferred_element_type=jnp.float32)
        return carry

    lax.fori_loop(0, STEPS, q_step, 0)
    for h in range(heads):
        q[h] = rotated(q_acc[:, h * HD:(h + 1) * HD])

    def score_block(j, own):
        ok = doc_q[...] == doc_all[j].astype(jnp.float32)
        if own:
            ok = ok & (lane <= lax.broadcasted_iota(jnp.int32, (rows, rows), 0))
        bias = jnp.where(ok, 0.0, -1e30).astype(jnp.float32)
        for h in range(kv_heads):
            s = lax.dot_general(
                q[h * group:(h + 1) * group].reshape(group * rows, HD),
                kv[j, :, h * HD:(h + 1) * HD],
                (((1,), (1,)), ((), ())), preferred_element_type=jnp.float32)
            s = (s.reshape(group, rows, rows) + bias[None]).reshape(group * rows, rows)
            sc[j, h] = s
            top[h] = s if own else jnp.maximum(top[h], s)

    score_block(me, True)

    def wait_block(j):
        for copy in block_copies(j, kv_fwd, 0, partner):
            copy.wait_recv()

    @pl.when(core == 1)
    def _():
        wait_block(me - 1)
        score_block(me - 1, False)

    def chip_step(i, carry):
        s = chip - 1 - i
        mine = s * 2 + core
        wait_block(mine)
        for copy in block_copies(mine, kv_fwd, s, partner):
            copy.start()
        score_block(mine, False)
        other = s * 2 + 1 - core
        wait_block(other)
        score_block(other, False)
        return carry

    lax.fori_loop(0, chip, chip_step, 0)

    factor = math.log2(math.e) / math.sqrt(HD)
    for h in range(kv_heads):
        top[h] = jnp.broadcast_to(jnp.max(top[h], axis=1, keepdims=True), top.shape[1:])
    tot[...] = jnp.zeros_like(tot)
    acc[...] = jnp.zeros_like(acc)

    def weigh(j, carry):
        for h in range(kv_heads):
            p = jnp.exp2((sc[j, h] - top[h]) * factor)
            tot[h] += p
            acc[h] += jnp.dot(
                p.astype(jnp.bfloat16), kv[j, :, kv_width + h * HD:kv_width + (h + 1) * HD],
                preferred_element_type=jnp.float32)
        return carry

    lax.fori_loop(0, me + 1, weigh, 0)
    for h in range(kv_heads):
        result = (acc[h] / jnp.sum(tot[h], axis=1, keepdims=True)).astype(jnp.bfloat16)
        for g in range(group):
            att[:, (h * group + g) * HD:(h * group + g + 1) * HD] = result[g * rows:(g + 1) * rows]

    def piece_copy(p, way):
        target = z + 1 if way == 0 else z - 1
        return pltpu.make_async_remote_copy(
            src_ref=part.at[p], dst_ref=rbuf.at[way, p],
            send_sem=part_send.at[p], recv_sem=part_recv.at[way, p],
            device_id={"head": target}, device_id_type=MESH)

    def project(k, carry):
        p = piece_of(k)
        wo_copy(p).wait()
        part[p] = jnp.dot(att[...], wo[p], preferred_element_type=jnp.float32).astype(jnp.bfloat16)

        @pl.when((z == 0) & (p >= SUB))
        def _():
            piece_copy(p, 0).start()

        @pl.when((z == n_head - 1) & (p < (n_head - 1) * SUB))
        def _():
            piece_copy(p, 1).start()
        return carry

    lax.fori_loop(0, n_head * SUB, project, 0)

    def pass_on(p, way):
        piece_copy(p, way).wait_recv()
        part[p] = (part[p].astype(jnp.float32) + rbuf[way, p].astype(jnp.float32)).astype(jnp.bfloat16)
        piece_copy(p, way).start()

    def relay(t, carry):
        a = t - z
        b = t - (n_head - 1 - z)

        @pl.when((z > 0) & (a >= 0) & (a < SUB * (n_head - 1 - z)))
        def _():
            pass_on(n_head * SUB - 1 - a, 0)

        @pl.when((z < n_head - 1) & (b >= 0) & (b < SUB * z))
        def _():
            pass_on(b, 1)
        return carry

    @pl.when((z > 0) & (z < n_head - 1))
    def _():
        lax.fori_loop(0, SUB * (n_head - 1) + n_head, relay, 0)

    def last(s, add_left, add_right):
        p = z * SUB + s
        value = part[p].astype(jnp.float32)
        if add_left:
            piece_copy(p, 0).wait_recv()
            value += rbuf[0, p].astype(jnp.float32)
        if add_right:
            piece_copy(p, 1).wait_recv()
            value += rbuf[1, p].astype(jnp.float32)
        out[:, s * piece:(s + 1) * piece] = value.astype(jnp.bfloat16)

    for which, left, right in ((z == 0, False, True), (z == n_head - 1, True, False),
                               ((z > 0) & (z < n_head - 1), True, True)):
        @pl.when(which)
        def _(left=left, right=right):
            for s in reversed(range(SUB)) if left else range(SUB):
                last(s, left, right)

    def drain_one(c, carry):
        for copy in block_copies(me, kv_send, c, c * 2 + core):
            copy.wait_send()
        return carry

    lax.fori_loop(chip + 1, chips, drain_one, 0)

    @pl.when(core == 0)
    def _():
        for copy in block_copies(me, kv_send, chip, partner):
            copy.wait_send()

    def drain_forward(s, carry):
        for copy in block_copies(s * 2 + core, kv_fwd, s, partner):
            copy.wait_send()
        return carry

    lax.fori_loop(0, chip, drain_forward, 0)

    def drain_piece(p, carry):
        @pl.when((p < z * SUB) | (p >= (z + 1) * SUB))
        def _():
            piece_copy(p, 0).wait_send()
        return carry

    lax.fori_loop(0, n_head * SUB, drain_piece, 0)


def solution(mesh):
    n_ctx, n_head = mesh.shape["ctx"], mesh.shape["head"]
    half = HD // 2
    base = 500000.0 ** (-2.0 * np.arange(half, dtype=np.float64) / HD)
    table = np.concatenate([base, base]).astype(np.float32)[None, :]

    def step(tokens, w_query, w_key, w_value, w_out, doc_ids):
        rows, width = tokens.shape
        q_width, kv_width = w_query.shape[1], w_key.shape[1]
        kv_heads, heads = kv_width // HD, q_width // HD
        group = heads // kv_heads
        step_rows = width // STEPS
        out_width = w_out.shape[1]
        pieces = n_head * SUB
        piece = out_width // pieces
        bf16, f32 = jnp.bfloat16, jnp.float32
        dma = pltpu.SemaphoreType.DMA
        return pl.pallas_call(
            functools.partial(kernel, n_ctx, n_head),
            out_shape=jax.ShapeDtypeStruct((rows, out_width // n_head), bf16),
            in_specs=[pl.BlockSpec(memory_space=pl.ANY)] * 7,
            out_specs=pl.BlockSpec(memory_space=pltpu.VMEM),
            scratch_shapes=[
                pltpu.VMEM((STEPS, rows, step_rows), bf16),
                pltpu.VMEM((STEPS, step_rows, q_width), bf16),
                pltpu.VMEM((STEPS, step_rows, kv_width), bf16),
                pltpu.VMEM((STEPS, step_rows, kv_width), bf16),
                pltpu.VMEM((pieces, q_width, piece), bf16),
                pltpu.VMEM((1, HD), f32),
                pltpu.VMEM((n_ctx, 1, rows), jnp.int32),
                pltpu.VMEM((n_ctx, rows, 2 * kv_width), bf16),
                pltpu.VMEM((rows, q_width), f32),
                pltpu.VMEM((rows, 2 * kv_width), f32),
                pltpu.VMEM((heads, rows, HD), bf16),
                pltpu.VMEM((rows, HD), f32),
                pltpu.VMEM((rows, HD), f32),
                pltpu.VMEM((rows, rows), f32),
                pltpu.VMEM((n_ctx, kv_heads, group * rows, rows), f32),
                pltpu.VMEM((kv_heads, group * rows, rows), f32),
                pltpu.VMEM((kv_heads, group * rows, rows), f32),
                pltpu.VMEM((kv_heads, group * rows, HD), f32),
                pltpu.VMEM((rows, q_width), bf16),
                pltpu.VMEM((pieces, rows, piece), bf16),
                pltpu.VMEM((2, pieces, rows, piece), bf16),
                dma((STEPS,)), dma((STEPS,)), dma((STEPS,)), dma((STEPS,)), dma((pieces,)), dma((2,)),
                dma((2, n_ctx // 2)), dma((2, n_ctx // 2)), dma((2, n_ctx)),
                dma((pieces,)), dma((2, pieces)),
            ],
            compiler_params=pltpu.CompilerParams(
                collective_id=0, has_side_effects=True, vmem_limit_bytes=60 * 1024 * 1024),
            name="attention_layer",
        )(tokens, w_query, w_key, w_value, w_out, doc_ids.reshape(1, rows), jnp.asarray(table))

    return jax.shard_map(
        step,
        mesh=mesh,
        in_specs=(
            P("ctx", None),
            P(None, "head"),
            P(None, "head"),
            P(None, "head"),
            P("head", None),
            P("ctx"),
        ),
        out_specs=P("ctx", "head"),
        check_vma=False,
    )
```

```python
import functools
import math

import jax
import jax.numpy as jnp
import numpy as np
from jax import lax
from jax.experimental import pallas as pl
from jax.experimental.pallas import tpu as pltpu
from jax.sharding import PartitionSpec as P

HD = 128
STEPS = 4
SUB = 2
PARTS = 2
MESH = pl.DeviceIdType.MESH


def kernel(
    n_ctx, n_head,
    tokens, w_query, w_key, w_value, w_out, docs, freqs, out,
    tok, wq, wk, wv, wo, freq, doc_all, keys, values, q_acc, k_acc, v_acc, q, cos_ref, sin_ref, doc_q,
    sc, top, tot, acc, att, part, rbuf,
    tok_sem, wq_sem, wk_sem, wv_sem, wo_sem, small_sem,
    kv_send, kv_fwd, kv_recv, part_send, part_recv,
):
    rows = tokens.shape[0]
    kv_heads = w_key.shape[1] // HD
    heads = w_query.shape[1] // HD
    group = heads // kv_heads
    part_rows = rows // PARTS
    chips = n_ctx // 2
    me = lax.axis_index("ctx")
    z = lax.axis_index("head")
    core = lax.rem(me, 2)
    chip = me // 2
    partner = me + 1 - 2 * core
    step_rows = wq.shape[1]
    piece = wo.shape[2]

    def tok_copy(c):
        return pltpu.make_async_copy(
            tokens.at[:, pl.ds(pl.multiple_of(c * step_rows, step_rows), step_rows)],
            tok.at[c], tok_sem.at[c])

    def rows_copy(src, dst, sem, c):
        return pltpu.make_async_copy(
            src.at[pl.ds(pl.multiple_of(c * step_rows, step_rows), step_rows), :],
            dst.at[c], sem.at[c])

    def wo_copy(p):
        return pltpu.make_async_copy(
            w_out.at[:, pl.ds(pl.multiple_of(p * piece, piece), piece)], wo.at[p], wo_sem.at[p])

    doc_copy = pltpu.make_async_copy(docs, doc_all.at[me], small_sem.at[0])
    freq_copy = pltpu.make_async_copy(freqs, freq, small_sem.at[1])

    def piece_of(k):
        return jnp.where(z < n_head // 2, n_head * SUB - 1 - k, k)

    doc_copy.start()
    freq_copy.start()
    for c in range(STEPS):
        tok_copy(c).start()
        rows_copy(w_key, wk, wk_sem, c).start()
    for c in range(STEPS):
        rows_copy(w_value, wv, wv_sem, c).start()

    barrier = pltpu.get_barrier_semaphore()

    def greet(c, carry):
        @pl.when(c != chip)
        def _():
            pl.semaphore_signal(
                barrier, inc=1, device_id={"ctx": c * 2 + core}, device_id_type=MESH)
        return carry

    lax.fori_loop(0, chips, greet, 0)
    pl.semaphore_signal(barrier, inc=1, device_id={"ctx": partner}, device_id_type=MESH)

    @pl.when(z > 0)
    def _():
        pl.semaphore_signal(barrier, inc=1, device_id={"head": z - 1}, device_id_type=MESH)

    @pl.when(z < n_head - 1)
    def _():
        pl.semaphore_signal(barrier, inc=1, device_id={"head": z + 1}, device_id_type=MESH)

    freq_copy.wait()
    doc_copy.wait()
    places = (me * rows + lax.broadcasted_iota(jnp.int32, (rows, HD), 0)).astype(jnp.float32)
    angles = places * freq[...]
    lane = lax.broadcasted_iota(jnp.int32, (rows, HD), 1)
    cos_ref[...] = jnp.cos(angles)
    sine = jnp.sin(angles)
    sin_ref[...] = jnp.where(lane < HD // 2, -sine, sine)
    doc_q[...] = jnp.broadcast_to(doc_all[me].astype(jnp.float32), (rows, rows)).T

    def rotated(x):
        return (x * cos_ref[...] + pltpu.roll(x, HD // 2, 1) * sin_ref[...]).astype(jnp.bfloat16)

    def copies(refs, block, sems, slot, target):
        return [
            pltpu.make_async_remote_copy(
                src_ref=ref.at[block], dst_ref=ref.at[block],
                send_sem=sems.at[i, slot], recv_sem=kv_recv.at[i, block],
                device_id={"ctx": target}, device_id_type=MESH)
            for i, ref in refs
        ]

    first, second = ((0, keys), (1, doc_all)), ((2, values),)

    def send_all(refs):
        def send_one(i, carry):
            c = chips - 1 - i
            for copy in copies(refs, me, kv_send, c, c * 2 + core):
                copy.start()
            return carry

        lax.fori_loop(0, chips - 1 - chip, send_one, 0)

        @pl.when(core == 0)
        def _():
            for copy in copies(refs, me, kv_send, chip, partner):
                copy.start()

    k_acc[...] = jnp.zeros_like(k_acc)

    def key_step(c, carry):
        tok_copy(c).wait()
        rows_copy(w_key, wk, wk_sem, c).wait()
        k_acc[...] += jnp.dot(tok[c], wk[c], preferred_element_type=jnp.float32)
        return carry

    lax.fori_loop(0, STEPS, key_step, 0)
    for h in range(kv_heads):
        keys[me, :, h * HD:(h + 1) * HD] = rotated(k_acc[:, h * HD:(h + 1) * HD])
    pl.semaphore_wait(
        barrier,
        chips + (z > 0).astype(jnp.int32) + (z < n_head - 1).astype(jnp.int32))
    send_all(first)

    v_acc[...] = jnp.zeros_like(v_acc)

    def value_step(c, carry):
        rows_copy(w_value, wv, wv_sem, c).wait()
        rows_copy(w_query, wq, wq_sem, c).start()
        v_acc[...] += jnp.dot(tok[c], wv[c], preferred_element_type=jnp.float32)
        return carry

    lax.fori_loop(0, STEPS, value_step, 0)
    values[me] = v_acc[...].astype(jnp.bfloat16)
    send_all(second)

    q_acc[...] = jnp.zeros_like(q_acc)

    def q_step(c, carry):
        rows_copy(w_query, wq, wq_sem, c).wait()
        for i in range(n_head * SUB // STEPS):
            wo_copy(piece_of(c * (n_head * SUB // STEPS) + i)).start()
        q_acc[...] += jnp.dot(tok[c], wq[c], preferred_element_type=jnp.float32)
        return carry

    lax.fori_loop(0, STEPS, q_step, 0)
    for h in range(heads):
        turned = rotated(q_acc[:, h * HD:(h + 1) * HD])
        for r in range(PARTS):
            q[h // group, r, h % group] = turned[r * part_rows:(r + 1) * part_rows]

    def score_block(j, own):
        ok = doc_q[...] == doc_all[j].astype(jnp.float32)
        if own:
            ok = ok & (lane <= lax.broadcasted_iota(jnp.int32, (rows, rows), 0))
        bias = jnp.where(ok, 0.0, -1e30).astype(jnp.float32)
        for h in range(kv_heads):
            s = lax.dot_general(
                q[h].reshape(group * rows, HD), keys[j, :, h * HD:(h + 1) * HD],
                (((1,), (1,)), ((), ())), preferred_element_type=jnp.float32)
            s = s.reshape(PARTS, group, part_rows, rows) + bias.reshape(PARTS, 1, part_rows, rows)
            s = s.reshape(PARTS, group * part_rows, rows)
            sc[j, h] = s
            top[h] = s if own else jnp.maximum(top[h], s)

    score_block(me, True)

    def wait_block(refs, j):
        for copy in copies(refs, j, kv_fwd, 0, partner):
            copy.wait_recv()

    def receive(refs, use):
        @pl.when(core == 1)
        def _():
            wait_block(refs, me - 1)
            use(me - 1)

        def chip_step(i, carry):
            s = chip - 1 - i
            mine = s * 2 + core
            wait_block(refs, mine)
            for copy in copies(refs, mine, kv_fwd, s, partner):
                copy.start()
            use(mine)
            other = s * 2 + 1 - core
            wait_block(refs, other)
            use(other)
            return carry

        lax.fori_loop(0, chip, chip_step, 0)

    receive(first, lambda j: score_block(j, False))
    receive(second, lambda j: None)

    factor = math.log2(math.e) / math.sqrt(HD)
    def attend(r):
        for h in range(kv_heads):
            top[h, r] = jnp.broadcast_to(
                jnp.max(top[h, r], axis=1, keepdims=True), top.shape[2:])
            tot[h] = jnp.zeros(tot.shape[1:], jnp.float32)
            acc[h] = jnp.zeros(acc.shape[1:], jnp.float32)

        def weigh(j, carry):
            for h in range(kv_heads):
                p = jnp.exp2((sc[j, h, r] - top[h, r]) * factor)
                tot[h] += p
                acc[h] += jnp.dot(
                    p.astype(jnp.bfloat16), values[j, :, h * HD:(h + 1) * HD],
                    preferred_element_type=jnp.float32)
            return carry

        lax.fori_loop(0, me + 1, weigh, 0)
        for h in range(kv_heads):
            result = (acc[h] / jnp.sum(tot[h], axis=1, keepdims=True)).astype(jnp.bfloat16)
            for g in range(group):
                att[r, :, (h * group + g) * HD:(h * group + g + 1) * HD] = (
                    result[g * part_rows:(g + 1) * part_rows])

    def piece_copy(r, p, way):
        target = z + 1 if way == 0 else z - 1
        return pltpu.make_async_remote_copy(
            src_ref=part.at[r, p], dst_ref=rbuf.at[way, r, p],
            send_sem=part_send.at[r, p], recv_sem=part_recv.at[way, r, p],
            device_id={"head": target}, device_id_type=MESH)

    def both(r, whole):
        attend(r)

        def project(k, carry):
            p = piece_of(k)

            @pl.when(r == 0)
            def _():
                wo_copy(p).wait()
            part[r, p] = jnp.dot(
                att[r], wo[p], preferred_element_type=jnp.float32).astype(jnp.bfloat16)

            @pl.when((z == 0) & (p >= SUB))
            def _():
                piece_copy(r, p, 0).start()

            @pl.when((z == n_head - 1) & (p < (n_head - 1) * SUB))
            def _():
                piece_copy(r, p, 1).start()
            return carry

        lax.fori_loop(0, n_head * SUB, project, 0)
        return whole

    lax.fori_loop(0, PARTS, both, 0)

    def pass_on(r, p, way):
        piece_copy(r, p, way).wait_recv()
        part[r, p] = (
            part[r, p].astype(jnp.float32) + rbuf[way, r, p].astype(jnp.float32)
        ).astype(jnp.bfloat16)
        piece_copy(r, p, way).start()

    def relay(r, t):
        a = t - z
        b = t - (n_head - 1 - z)

        @pl.when((z > 0) & (a >= 0) & (a < SUB * (n_head - 1 - z)))
        def _():
            pass_on(r, n_head * SUB - 1 - a, 0)

        @pl.when((z < n_head - 1) & (b >= 0) & (b < SUB * z))
        def _():
            pass_on(r, b, 1)

    length = SUB * (n_head - 1) + n_head

    def relay_step(i, carry):
        relay(i // length, lax.rem(i, length))
        return carry

    @pl.when((z > 0) & (z < n_head - 1))
    def _():
        lax.fori_loop(0, PARTS * length, relay_step, 0)

    def last(r, s, add_left, add_right):
        p = z * SUB + s
        value = part[r, p].astype(jnp.float32)
        if add_left:
            piece_copy(r, p, 0).wait_recv()
            value += rbuf[0, r, p].astype(jnp.float32)
        if add_right:
            piece_copy(r, p, 1).wait_recv()
            value += rbuf[1, r, p].astype(jnp.float32)
        out[r * part_rows:(r + 1) * part_rows, s * piece:(s + 1) * piece] = (
            value.astype(jnp.bfloat16))

    for which, left, right in ((z == 0, False, True), (z == n_head - 1, True, False),
                               ((z > 0) & (z < n_head - 1), True, True)):
        @pl.when(which)
        def _(left=left, right=right):
            for r in range(PARTS):
                for s in reversed(range(SUB)) if left else range(SUB):
                    last(r, s, left, right)

    everything = first + second

    def drain_one(c, carry):
        for copy in copies(everything, me, kv_send, c, c * 2 + core):
            copy.wait_send()
        return carry

    lax.fori_loop(chip + 1, chips, drain_one, 0)

    @pl.when(core == 0)
    def _():
        for copy in copies(everything, me, kv_send, chip, partner):
            copy.wait_send()

    def drain_forward(s, carry):
        for copy in copies(everything, s * 2 + core, kv_fwd, s, partner):
            copy.wait_send()
        return carry

    lax.fori_loop(0, chip, drain_forward, 0)

    def drain_piece(p, carry):
        @pl.when((p < z * SUB) | (p >= (z + 1) * SUB))
        def _():
            for r in range(PARTS):
                piece_copy(r, p, 0).wait_send()
        return carry

    lax.fori_loop(0, n_head * SUB, drain_piece, 0)


def solution(mesh):
    n_ctx, n_head = mesh.shape["ctx"], mesh.shape["head"]
    half = HD // 2
    base = 500000.0 ** (-2.0 * np.arange(half, dtype=np.float64) / HD)
    table = np.concatenate([base, base]).astype(np.float32)[None, :]

    def step(tokens, w_query, w_key, w_value, w_out, doc_ids):
        rows, width = tokens.shape
        q_width, kv_width = w_query.shape[1], w_key.shape[1]
        kv_heads, heads = kv_width // HD, q_width // HD
        group = heads // kv_heads
        step_rows = width // STEPS
        part_rows = rows // PARTS
        out_width = w_out.shape[1]
        pieces = n_head * SUB
        piece = out_width // pieces
        bf16, f32 = jnp.bfloat16, jnp.float32
        dma = pltpu.SemaphoreType.DMA
        return pl.pallas_call(
            functools.partial(kernel, n_ctx, n_head),
            out_shape=jax.ShapeDtypeStruct((rows, out_width // n_head), bf16),
            in_specs=[pl.BlockSpec(memory_space=pl.ANY)] * 7,
            out_specs=pl.BlockSpec(memory_space=pltpu.VMEM),
            scratch_shapes=[
                pltpu.VMEM((STEPS, rows, step_rows), bf16),
                pltpu.VMEM((STEPS, step_rows, q_width), bf16),
                pltpu.VMEM((STEPS, step_rows, kv_width), bf16),
                pltpu.VMEM((STEPS, step_rows, kv_width), bf16),
                pltpu.VMEM((pieces, q_width, piece), bf16),
                pltpu.VMEM((1, HD), f32),
                pltpu.VMEM((n_ctx, 1, rows), jnp.int32),
                pltpu.VMEM((n_ctx, rows, kv_width), bf16),
                pltpu.VMEM((n_ctx, rows, kv_width), bf16),
                pltpu.VMEM((rows, q_width), f32),
                pltpu.VMEM((rows, kv_width), f32),
                pltpu.VMEM((rows, kv_width), f32),
                pltpu.VMEM((kv_heads, PARTS, group, rows // PARTS, HD), bf16),
                pltpu.VMEM((rows, HD), f32),
                pltpu.VMEM((rows, HD), f32),
                pltpu.VMEM((rows, rows), f32),
                pltpu.VMEM((n_ctx, kv_heads, PARTS, group * part_rows, rows), f32),
                pltpu.VMEM((kv_heads, PARTS, group * part_rows, rows), f32),
                pltpu.VMEM((kv_heads, group * part_rows, rows), f32),
                pltpu.VMEM((kv_heads, group * part_rows, HD), f32),
                pltpu.VMEM((PARTS, part_rows, q_width), bf16),
                pltpu.VMEM((PARTS, pieces, part_rows, piece), bf16),
                pltpu.VMEM((2, PARTS, pieces, part_rows, piece), bf16),
                dma((STEPS,)), dma((STEPS,)), dma((STEPS,)), dma((STEPS,)), dma((pieces,)), dma((2,)),
                dma((3, n_ctx // 2)), dma((3, n_ctx // 2)), dma((3, n_ctx)),
                dma((PARTS, pieces)), dma((2, PARTS, pieces)),
            ],
            compiler_params=pltpu.CompilerParams(
                collective_id=0, has_side_effects=True, vmem_limit_bytes=60 * 1024 * 1024),
            name="attention_layer",
        )(tokens, w_query, w_key, w_value, w_out, doc_ids.reshape(1, rows), jnp.asarray(table))

    return jax.shard_map(
        step,
        mesh=mesh,
        in_specs=(
            P("ctx", None),
            P(None, "head"),
            P(None, "head"),
            P(None, "head"),
            P("head", None),
            P("ctx"),
        ),
        out_specs=P("ctx", "head"),
        check_vma=False,
    )
```
